32 devices in a mesh: chain: 8 (over y, x, core), par: 4 (over z).
Axes of the slice: x: 2, y: 2, z: 4, core: 2. Of those that a mesh axis runs over, the one named last changes fastest.
Arguments:
- propagation_gains: bfloat16 [4, 16, 64, 8192], P('par', None, None, 'chain'), may hold values from -0.13258252 to 0.13258252, as said below
- observed_samples: bfloat16 [4, 16, 32, 8192], P('par', None, None, 'chain'), may hold values from -6 to 6
- disturbance_variance: float32 [4, 16], P(None, 'chain'), may hold values from 0.05 to 0.5
- retained_branches: int32 [4, 16, 16, 1024], P(None, 'chain', 'par'), may hold values from 0 to 63
Outputs:
- distances: float32 [4, 16, 16, 1024], P(None, 'chain', 'par')
The draws below stay inside these ranges and needn't reach their ends.
Inputs may be any that keep to these rules, and one draw needn't show every extreme that they name: `propagation_gains`: row 2u holds the real and row 2u+1 the imaginary part of the channel to user u.
All inputs are finite; a program needn't handle non-finite values.
Results may differ from the reference program's by a relative error of at most 0.0003.
Values sent between devices are 32-bit elements; how exact they have to be, the bound alone decides.
A program may use at most 64 MiB of HBM per device.

```python
import math
import jax
import jax.numpy as jnp
from jax import lax

TERMINAL_NUMBER = 32
KEPT_BRANCHES = 32
FREQ_GROUP_NUM = 4
TONES_PER_GROUP = 16
SLOTS_PER_FRAME = 16
ANTENNA_TOTAL = 8192


def draw_propagation_gains(key, part):
    base = jax.random.fold_in(key, 11)
    private_key, common_key, key_gain = jax.random.split(base, 3)
    common_weight = 0.5
    gain_low = 0.5
    gain_high = 2.0
    private_part = jnp.clip(jax.random.normal(private_key, (FREQ_GROUP_NUM, TONES_PER_GROUP, 2 * TERMINAL_NUMBER, ANTENNA_TOTAL), jnp.float32), -4.0, 4.0)
    common_part = jnp.clip(jax.random.normal(common_key, (FREQ_GROUP_NUM, TONES_PER_GROUP, 2, ANTENNA_TOTAL), jnp.float32), -4.0, 4.0)
    shared = jnp.tile(common_part, (1, 1, TERMINAL_NUMBER, 1))
    log_gain = jax.random.uniform(key_gain, (FREQ_GROUP_NUM, TONES_PER_GROUP, TERMINAL_NUMBER, 1), jnp.float32, math.log(gain_low), math.log(gain_high))
    gains = jnp.repeat(jnp.exp(log_gain), 2, axis=2)
    factor_matrix = 1.0 / math.sqrt(2.0 * ANTENNA_TOTAL * (1.0 + common_weight * common_weight))
    return (gains * (private_part + common_weight * shared) * factor_matrix).astype(jnp.bfloat16)


def touch_ends(drawn, stream_key, least, high):
    longest = drawn.shape.index(max(drawn.shape))
    spots = []
    for shift in (0, 1):
        where = [jax.random.randint(jax.random.fold_in(stream_key, axis), (), 0, length) for axis, length in enumerate(drawn.shape)]
        where[longest] = (where[longest] + shift) % drawn.shape[longest]
        spots.append(tuple(where))
    return drawn.at[spots[0]].set(least).at[spots[1]].set(high)


def levels(own_key, dims, cuts, least, high):
    def one(dim, shards_of):
        heights = jax.random.uniform(jax.random.fold_in(jax.random.fold_in(own_key, 6), dim), (shards_of,), jnp.float32, least / len(cuts), high / len(cuts))
        return jnp.repeat(jnp.exp(heights), dims[dim] // shards_of).reshape((-1,) + (1,) * (len(dims) - dim - 1))

    factor_of = one(*cuts[0])
    for cut in cuts[1:]:
        factor_of = factor_of * one(*cut)
    return factor_of


def scatter_about(stream_key, shape, deviation, bound, shards=(), kind=jnp.bfloat16):
    level = levels(stream_key, shape, shards, -0.22, 0.18) if shards else 1.0
    result = jax.random.normal(stream_key, shape, jnp.float32) * deviation * level
    return jnp.minimum(jnp.maximum(result, -bound), bound).astype(kind)


def setup_inputs(seed: int = 0) -> dict:
    keys = jax.random.split(jax.random.key(seed), 5)
    return {
        "propagation_gains": draw_propagation_gains(jax.random.fold_in(keys[4], 71), 0),
        "observed_samples": scatter_about(keys[1], (FREQ_GROUP_NUM, TONES_PER_GROUP, 2 * SLOTS_PER_FRAME, ANTENNA_TOTAL), 1.0, 6.0, ((0, 4), (3, 8))),
        "disturbance_variance": jnp.clip(jnp.exp(math.log(0.5) - 2.3025851 * jax.random.uniform(keys[2], (FREQ_GROUP_NUM, TONES_PER_GROUP), jnp.float32) ** levels(keys[2], (FREQ_GROUP_NUM, TONES_PER_GROUP), ((1, 8),), -0.2, 0.2)), 0.05, 0.5),
        "retained_branches": touch_ends(jax.random.randint(keys[3], (FREQ_GROUP_NUM, TONES_PER_GROUP, SLOTS_PER_FRAME, KEPT_BRANCHES * TERMINAL_NUMBER), 0, 64), jax.random.fold_in(keys[3], 1), 0, 63).astype(jnp.int32),
    }


constellation_norm = 1.0 / 42.0 ** 0.5

def fold_stats(raw_gram, raw_cross):
    outer_dimensions = raw_gram.shape[:-2]
    terminal_number = raw_gram.shape[-1] // 2
    pieces = raw_gram.reshape(outer_dimensions + (terminal_number, 2, terminal_number, 2))
    same_part = pieces[..., :, 0, :, 0] + pieces[..., :, 1, :, 1]
    cross_part = pieces[..., :, 1, :, 0] - pieces[..., :, 0, :, 1]
    crossed = raw_cross.reshape(outer_dimensions + (terminal_number, 2, -1, 2))
    rhs_real = crossed[..., :, 0, :, 0] + crossed[..., :, 1, :, 1]
    rhs_imag = crossed[..., :, 0, :, 1] - crossed[..., :, 1, :, 0]
    rhs = jnp.stack([rhs_real, rhs_imag], axis=-2).reshape(outer_dimensions + (2 * terminal_number, -1))
    return (same_part, cross_part, rhs)

def assemble(same_part, cross_part, noise):
    row_even = jnp.stack([same_part, cross_part], axis=-1)
    row_odd = jnp.stack([-cross_part, same_part], axis=-1)
    whole = jnp.stack([row_even, row_odd], axis=-3)
    order = 2 * same_part.shape[-1]
    gram = whole.reshape(same_part.shape[:-2] + (order, order))
    return gram + noise[..., None, None] * jnp.eye(order, dtype=jnp.float32)

def estimate_transmitted(cholesky_triangle, whitened_observation, retained_branches):
    terminal_number = cholesky_triangle.shape[-1] // 2
    outer_dimensions = retained_branches.shape[:-1]
    kept_branch_number = retained_branches.shape[-1] // terminal_number
    constellation_position = retained_branches.reshape(outer_dimensions + (kept_branch_number, terminal_number))
    inphase_amplitude = (2 * (constellation_position % 8) - 7).astype(jnp.float32)
    quadrature_amplitude = (2 * (constellation_position // 8) - 7).astype(jnp.float32)
    branch_vector = jnp.stack([inphase_amplitude, quadrature_amplitude], axis=-1).reshape(outer_dimensions + (kept_branch_number, 2 * terminal_number)) * constellation_norm
    upper_factor = jnp.swapaxes(cholesky_triangle, -1, -2)
    mapped = jnp.einsum('bsij,bstkj->bstki', upper_factor, branch_vector, precision=lax.Precision.HIGHEST)
    remainder_error = jnp.swapaxes(whitened_observation, -1, -2)[..., None, :] - mapped
    squared_errors = (remainder_error * remainder_error).reshape(outer_dimensions + (kept_branch_number, terminal_number, 2)).sum(axis=-1)
    accrued_metric = jnp.cumsum(squared_errors[..., ::-1], axis=-1)[..., ::-1] / terminal_number
    return accrued_metric.reshape(outer_dimensions + (kept_branch_number * terminal_number,))

def reference(propagation_gains, observed_samples, disturbance_variance, retained_branches):

    def band_stats(inputs):
        chan_band, recv_band = inputs
        chan_f = chan_band.astype(jnp.float32)
        recv_f = recv_band.astype(jnp.float32)
        gram_band = jnp.einsum('sra,sqa->srq', chan_f, chan_f, precision=lax.Precision.HIGHEST)
        cross_band = jnp.einsum('sra,sqa->srq', chan_f, recv_f, precision=lax.Precision.HIGHEST)
        return (gram_band, cross_band)
    raw_gram, raw_cross = lax.map(band_stats, (propagation_gains, observed_samples))
    same_part, cross_part, rhs = fold_stats(raw_gram, raw_cross)
    gram = assemble(same_part, cross_part, disturbance_variance)
    cholesky_triangle = jnp.linalg.cholesky(gram)
    whitened_observation = jax.scipy.linalg.solve_triangular(cholesky_triangle, rhs, lower=True)
    return estimate_transmitted(cholesky_triangle, whitened_observation, retained_branches)
```

```python
import functools
import jax
import jax.numpy as jnp
from jax import lax
from jax.experimental import pallas as pl
from jax.experimental.pallas import tpu as pltpu
from jax.sharding import PartitionSpec as P

constellation_norm = 1.0 / 42.0**0.5
LANES = 128
MESH = pl.DeviceIdType.MESH
NT = (((1,), (1,)), ((), ()))


def iota(shape, dim):
    return lax.broadcasted_iota(jnp.int32, shape, dim)


def split(x):
    high = x.astype(jnp.bfloat16)
    return high, (x - high.astype(jnp.float32)).astype(jnp.bfloat16)


def pair_swap(x):
    even = iota(x.shape, 1) % 2 == 0
    return jnp.where(even, pltpu.roll(x, LANES - 1, 1), pltpu.roll(x, 1, 1))


def eliminate(mats, users):
    groups = users // 8
    blocks, turned = [], []
    for mat in mats:
        odd = iota((8, LANES), 1) % 2 == 1
        parts = [mat[8 * g : 8 * g + 8, :] for g in range(groups)]
        blocks.append(parts)
        turned.append([jnp.where(odd, pair_swap(p), -pair_swap(p)) for p in parts])
    row = iota((8, LANES), 0)
    for j in range(users - 1):
        home, at = divmod(j, 8)
        for a, ia in zip(blocks, turned):
            pivot_row, turned_row = a[home][at : at + 1, :], ia[home][at : at + 1, :]
            inverse = 1.0 / pivot_row[:, 2 * j : 2 * j + 1]
            pivot_row, turned_row = pivot_row * inverse, turned_row * inverse
            for g in range(home + (at == 7), groups):
                real = jnp.broadcast_to(a[g][:, 2 * j : 2 * j + 1], (8, LANES))
                imag = jnp.broadcast_to(a[g][:, 2 * j + 1 : 2 * j + 2], (8, LANES))
                if g == home:
                    real = jnp.where(row > at, real, 0.0)
                    imag = jnp.where(row > at, imag, 0.0)
                a[g] = a[g] - (real * pivot_row + imag * turned_row)
                ia[g] = ia[g] - (real * turned_row - imag * pivot_row)
    lane, line = iota((users, LANES), 1), iota((users, LANES), 0)
    keep = (lane >= 2 * line) & (lane != 2 * line + 1) | (lane >= 2 * users)
    out = []
    for a in blocks:
        full = jnp.concatenate(a, axis=0)
        pivots = jnp.sum(jnp.where(lane == 2 * line, full, 0.0), axis=1, keepdims=True)
        out.append(jnp.where(keep, full * lax.rsqrt(pivots), 0.0))
    return out


def kernel(
    dims, noise_ref, gains_ref, samples_ref, branches_ref, out_ref,
    held, raw, part, came, points, packed, taken, rotations,
    load_sem, send_sem, recv_sem, usend_sem, urecv_sem,
):
    clusters, bands, users, symbols, share, mine_t, pieces = dims
    copies = LANES // users
    lines = pieces * mine_t
    me, band = lax.axis_index("chain"), lax.axis_index("par")

    barrier = pltpu.get_barrier_semaphore()
    for k in range(1, clusters):
        pl.semaphore_signal(barrier, inc=1, device_id={"chain": lax.rem(me + k, clusters)}, device_id_type=MESH)
    for k in range(1, bands):
        pl.semaphore_signal(barrier, inc=1, device_id={"par": lax.rem(band + k, bands)}, device_id_type=MESH)

    order = list(range(1, clusters)) + [0]
    loads = {}
    for k in order:
        tones = pl.ds(lax.rem(me + k, clusters) * share, share)
        loads[k] = (
            pltpu.make_async_copy(
                gains_ref.at[0, tones], held.at[k, :, pl.ds(0, 2 * users)], load_sem.at[0, k]
            ),
            pltpu.make_async_copy(
                samples_ref.at[0, tones], held.at[k, :, pl.ds(2 * users, 2 * symbols)], load_sem.at[1, k]
            ),
        )
        for copy in loads[k]:
            copy.start()

    raw[...] = jnp.zeros_like(raw)
    even = iota((users, LANES), 1) % 2 == 0
    sends = []
    for number, k in enumerate(order):
        for copy in loads[k]:
            copy.wait()
        for s in range(share):
            slot = (number * share + s) % raw.shape[0]
            both = held[k, s]
            raw[slot, :, : 2 * (users + symbols)] = lax.dot_general(
                both[: 2 * users], both, NT, preferred_element_type=jnp.float32
            )
            on_even = raw[slot, pl.ds(0, users, stride=2), :]
            on_odd = raw[slot, pl.ds(1, users, stride=2), :]
            part[k, s] = pair_swap(on_odd) + jnp.where(even, on_even, -on_even)
        if k:
            if number == 0:
                pl.semaphore_wait(barrier, clusters + bands - 2)
            copy = pltpu.make_async_remote_copy(
                src_ref=part.at[k], dst_ref=came.at[k], send_sem=send_sem.at[k], recv_sem=recv_sem.at[k],
                device_id={"chain": lax.rem(me + k, clusters)}, device_id_type=MESH,
            )
            copy.start()
            sends.append(copy)

    for b in range(bands):
        for s in range(share):
            q = jnp.concatenate(
                [branches_ref[b, s, :, LANES * r : LANES * (r + 1)] for r in range(pieces)], axis=0
            )
            points[b, s, :, :LANES] = (2 * (q & 7) - 7).astype(jnp.float32).astype(jnp.bfloat16)
            points[b, s, :, LANES:] = (2 * (q >> 3) - 7).astype(jnp.float32).astype(jnp.bfloat16)

    lane, line = iota((users, LANES), 1), iota((users, LANES), 0)
    totals = [part[0, s] for s in range(share)]
    for copy in sends:
        copy.wait_recv()
    for k in range(1, clusters):
        totals = [total + came[k, s] for s, total in enumerate(totals)]
    mats = [
        jnp.where(lane == 2 * line, total + noise_ref[band, s], total) for s, total in enumerate(totals)
    ]
    factors = eliminate(mats, users)

    source, target = iota((LANES, LANES), 0), iota((LANES, LANES), 1) % (2 * users)
    spread = (source == 2 * (target % users) + target // users).astype(jnp.float32).astype(jnp.bfloat16)
    rows = 2 * mine_t
    r, c = iota((bands * rows, LANES), 0), iota((bands * rows, LANES), 1)
    is_odd = (r % rows) // mine_t
    wanted = 2 * users + 2 * ((r // rows) * mine_t + r % mine_t) + is_odd
    pick = jnp.where(c == wanted, (1 - 2 * is_odd).astype(jnp.float32), 0.0).astype(jnp.bfloat16)
    pick = jnp.concatenate([pick, pick], axis=1)
    half = users // 2
    left = iota((half, LANES), 1) < 2 * users
    for s, factor in enumerate(factors):
        high, low = split(factor * constellation_norm)
        wide = jnp.dot(high, spread, preferred_element_type=jnp.float32) + jnp.dot(
            low, spread, preferred_element_type=jnp.float32
        )
        folded = jnp.where(left, wide[:half], wide[half:])
        for k in range(bands):
            packed[k, s, :half] = folded
        high, low = split(factor)
        weights = jnp.concatenate(
            [jnp.concatenate([high] * copies, axis=0), jnp.concatenate([low] * copies, axis=0)], axis=1
        )
        rotations[s] = lax.dot_general(pick, weights, NT, preferred_element_type=jnp.float32)
        for k in range(bands):
            peer = lax.rem(band + k, bands)
            packed[k, s, half:] = rotations[s, pl.ds(pl.multiple_of(peer * rows, rows), rows), :]
    usends = []
    for k in range(1, bands):
        copy = pltpu.make_async_remote_copy(
            src_ref=packed.at[k], dst_ref=taken.at[k], send_sem=usend_sem.at[k], recv_sem=urecv_sem.at[k],
            device_id={"par": lax.rem(band + k, bands)}, device_id_type=MESH,
        )
        copy.start()
        usends.append(copy)

    sr, sc = iota((LANES, LANES), 0), iota((LANES, LANES), 1)
    suffix = jnp.where((sr // users == sc // users) & (sr >= sc), 1.0 / users, 0.0).astype(jnp.bfloat16)
    suffix = jnp.concatenate([suffix, suffix], axis=0)
    lane_block = lane // users
    for k in range(bands):
        if k:
            usends[k - 1].wait_recv()
        b = lax.rem(band + bands - k, bands)
        box = taken if k else packed
        for s in range(share):
            folded = box[k, s, :half]
            crossed = pltpu.roll(folded, 2 * users, 1)
            first = jnp.concatenate(
                [jnp.where(left, folded, crossed), jnp.where(left, crossed, folded)], axis=0
            )
            second = pltpu.roll(first, users, 1)
            ons, offs = [], []
            for i in range(copies):
                here = lane_block == i
                real, imag = (first, second) if i % 2 == 0 else (second, first)
                real, imag = jnp.where(here, real, 0.0), jnp.where(here, imag, 0.0)
                ons.append(jnp.concatenate([real, imag], axis=1))
                offs.append(jnp.concatenate([-imag, real], axis=1))
            high, low = split(jnp.concatenate(ons + offs, axis=0))
            p = points[b, s]
            mapped = lax.dot_general(p, high, NT, preferred_element_type=jnp.float32) + lax.dot_general(
                p, low, NT, preferred_element_type=jnp.float32
            )
            on = jnp.concatenate([box[k, s, half : half + mine_t]] * pieces, axis=0) - mapped[:, :LANES]
            off = jnp.concatenate([box[k, s, half + mine_t :]] * pieces, axis=0) - mapped[:, LANES:]
            high, low = split(on * on + off * off)
            result = jnp.dot(
                jnp.concatenate([high, low], axis=1), suffix, preferred_element_type=jnp.float32
            )
            for r in range(pieces):
                out_ref[b, s, :, LANES * r : LANES * (r + 1)] = result[mine_t * r : mine_t * (r + 1)]
    for copy in sends + usends:
        copy.wait_send()


def local(propagation_gains, observed_samples, disturbance_variance, retained_branches):
    clusters, bands = lax.axis_size("chain"), lax.axis_size("par")
    _, tones, double_users, antennas = propagation_gains.shape
    users, symbols = double_users // 2, observed_samples.shape[2] // 2
    share, mine_t = tones // clusters, symbols // bands
    pieces = retained_branches.shape[-1] // LANES
    dims = (clusters, bands, users, symbols, share, mine_t, pieces)
    f32, bf16 = jnp.float32, jnp.bfloat16
    vmem, dma = pltpu.VMEM, pltpu.SemaphoreType.DMA
    payload = users // 2 + 2 * mine_t
    return pl.pallas_call(
        functools.partial(kernel, dims),
        out_shape=jax.ShapeDtypeStruct(retained_branches.shape, f32),
        in_specs=[
            pl.BlockSpec(memory_space=pltpu.SMEM),
            pl.BlockSpec(memory_space=pl.ANY),
            pl.BlockSpec(memory_space=pl.ANY),
            pl.BlockSpec(memory_space=pltpu.VMEM),
        ],
        out_specs=pl.BlockSpec(memory_space=pltpu.VMEM),
        scratch_shapes=[
            vmem((clusters, share, 2 * (users + symbols), antennas), bf16),
            vmem((4, 2 * users, LANES), f32),
            vmem((clusters, share, users, LANES), f32),
            vmem((clusters, share, users, LANES), f32),
            vmem((bands, share, pieces * mine_t, 2 * LANES), bf16),
            vmem((bands, share, payload, LANES), f32),
            vmem((bands, share, payload, LANES), f32),
            vmem((share, bands * 2 * mine_t, LANES), f32),
            dma((2, clusters)), dma((clusters,)), dma((clusters,)), dma((bands,)), dma((bands,)),
        ],
        compiler_params=pltpu.CompilerParams(collective_id=0, has_side_effects=True),
        name="detect",
    )(disturbance_variance, propagation_gains, observed_samples, retained_branches)


def solution(mesh):
    placed = (
        P("par", None, None, "chain"),
        P("par", None, None, "chain"),
        P(None, "chain"),
        P(None, "chain", "par", None),
    )
    return jax.shard_map(
        local, mesh=mesh, in_specs=placed, out_specs=P(None, "chain", "par", None), check_vma=False
    )
```

```python
import functools
import jax
import jax.numpy as jnp
from jax import lax
from jax.experimental import pallas as pl
from jax.experimental.pallas import tpu as pltpu
from jax.sharding import PartitionSpec as P

constellation_norm = 1.0 / 42.0**0.5
LANES = 128
PANEL = 4
MESH = pl.DeviceIdType.MESH
NT = (((1,), (1,)), ((), ()))


def iota(shape, dim):
    return lax.broadcasted_iota(jnp.int32, shape, dim)


def split(x):
    high = x.astype(jnp.bfloat16)
    return high, (x - high.astype(jnp.float32)).astype(jnp.bfloat16)


def pair_swap(x):
    even = iota(x.shape, 1) % 2 == 0
    return jnp.where(even, pltpu.roll(x, LANES - 1, 1), pltpu.roll(x, 1, 1))


def eliminate(mats, users):
    groups = users // 8
    blocks, turned = [], []
    for mat in mats:
        odd = iota((8, LANES), 1) % 2 == 1
        parts = [mat[8 * g : 8 * g + 8, :] for g in range(groups)]
        blocks.append(parts)
        turned.append([jnp.where(odd, pair_swap(p), -pair_swap(p)) for p in parts])
    row = iota((8, LANES), 0)
    for start in range(0, users, PANEL):
        home = start // 8
        panels = [
            [
                {g: jnp.broadcast_to(a[g][:, lane : lane + 1], (8, LANES)) for g in range(home, groups)}
                for lane in range(2 * start, 2 * (start + PANEL))
            ]
            for a in blocks
        ]
        for j in range(start, min(start + PANEL, users - 1)):
            at, c = j % 8, j - start
            for a, ia, panel in zip(blocks, turned, panels):
                real, imag = panel[2 * c], panel[2 * c + 1]
                inverse = 1.0 / real[home][at : at + 1, :]
                pivot_row = a[home][at : at + 1, :] * inverse
                turned_row = ia[home][at : at + 1, :] * inverse
                later = [
                    (d, real[home][at + d - c : at + d - c + 1, :] * inverse, imag[home][at + d - c : at + d - c + 1, :] * inverse)
                    for d in range(c + 1, PANEL)
                ]
                for g in range(home + (at == 7), groups):
                    fr, fi = real[g], imag[g]
                    if g == home:
                        fr, fi = jnp.where(row > at, fr, 0.0), jnp.where(row > at, fi, 0.0)
                    for d, x, y in later:
                        panel[2 * d][g] = panel[2 * d][g] - (fr * x + fi * y)
                        panel[2 * d + 1][g] = panel[2 * d + 1][g] - (fi * x - fr * y)
                    a[g] = a[g] - (fr * pivot_row + fi * turned_row)
                    ia[g] = ia[g] - (fr * turned_row - fi * pivot_row)
    lane, line = iota((users, LANES), 1), iota((users, LANES), 0)
    keep = (lane >= 2 * line) & (lane != 2 * line + 1) | (lane >= 2 * users)
    out = []
    for a in blocks:
        full = jnp.concatenate(a, axis=0)
        pivots = jnp.sum(jnp.where(lane == 2 * line, full, 0.0), axis=1, keepdims=True)
        out.append(jnp.where(keep, full * lax.rsqrt(pivots), 0.0))
    return out


def kernel(
    dims, noise_any, gains_ref, samples_ref, branches_any, out_ref,
    noise_ref, branches_ref, held, raw, part, came, points, packed, taken, rotations,
    small_sem, load_sem, send_sem, recv_sem, usend_sem, urecv_sem,
):
    clusters, bands, users, symbols, share, mine_t, pieces = dims
    copies = LANES // users
    lines = pieces * mine_t
    me, band = lax.axis_index("chain"), lax.axis_index("par")

    barrier = pltpu.get_barrier_semaphore()
    for k in range(1, clusters):
        pl.semaphore_signal(barrier, inc=1, device_id={"chain": lax.rem(me + k, clusters)}, device_id_type=MESH)
    for k in range(1, bands):
        pl.semaphore_signal(barrier, inc=1, device_id={"par": lax.rem(band + k, bands)}, device_id_type=MESH)

    order = list(range(1, clusters)) + [0]
    loads = {}
    for k in order:
        tones = pl.ds(lax.rem(me + k, clusters) * share, share)
        loads[k] = (
            pltpu.make_async_copy(
                gains_ref.at[0, tones], held.at[k, :, pl.ds(0, 2 * users)], load_sem.at[0, k]
            ),
            pltpu.make_async_copy(
                samples_ref.at[0, tones], held.at[k, :, pl.ds(2 * users, 2 * symbols)], load_sem.at[1, k]
            ),
        )
        for copy in loads[k]:
            copy.start()

    small = (
        pltpu.make_async_copy(noise_any, noise_ref, small_sem.at[0]),
        pltpu.make_async_copy(branches_any, branches_ref, small_sem.at[1]),
    )
    for copy in small:
        copy.start()
    raw[...] = jnp.zeros_like(raw)
    even = iota((users, LANES), 1) % 2 == 0
    sends = []
    for number, k in enumerate(order):
        for copy in loads[k]:
            copy.wait()
        for s in range(share):
            slot = (number * share + s) % raw.shape[0]
            both = held[k, s]
            raw[slot, :, : 2 * (users + symbols)] = lax.dot_general(
                both[: 2 * users], both, NT, preferred_element_type=jnp.float32
            )
            on_even = raw[slot, pl.ds(0, users, stride=2), :]
            on_odd = raw[slot, pl.ds(1, users, stride=2), :]
            part[k, s] = pair_swap(on_odd) + jnp.where(even, on_even, -on_even)
        if k:
            if number == 0:
                pl.semaphore_wait(barrier, clusters + bands - 2)
            copy = pltpu.make_async_remote_copy(
                src_ref=part.at[k], dst_ref=came.at[k], send_sem=send_sem.at[k], recv_sem=recv_sem.at[k],
                device_id={"chain": lax.rem(me + k, clusters)}, device_id_type=MESH,
            )
            copy.start()
            sends.append(copy)

    for copy in small:
        copy.wait()
    for b in range(bands):
        for s in range(share):
            q = jnp.concatenate(
                [branches_ref[b, s, :, LANES * r : LANES * (r + 1)] for r in range(pieces)], axis=0
            )
            points[b, s, :, :LANES] = (2 * (q & 7) - 7).astype(jnp.float32).astype(jnp.bfloat16)
            points[b, s, :, LANES:] = (2 * (q >> 3) - 7).astype(jnp.float32).astype(jnp.bfloat16)

    lane, line = iota((users, LANES), 1), iota((users, LANES), 0)
    noises = [
        jnp.sum(jnp.where(iota((1, bands), 1) == band, noise_ref[s : s + 1, :], 0.0), axis=1, keepdims=True)
        for s in range(share)
    ]
    totals = [part[0, s] for s in range(share)]
    for copy in sends:
        copy.wait_recv()
    for k in range(1, clusters):
        totals = [total + came[k, s] for s, total in enumerate(totals)]
    mats = [
        jnp.where(lane == 2 * line, total + noises[s], total) for s, total in enumerate(totals)
    ]
    factors = eliminate(mats, users)

    source, target = iota((LANES, LANES), 0), iota((LANES, LANES), 1) % (2 * users)
    spread = (source == 2 * (target % users) + target // users).astype(jnp.float32).astype(jnp.bfloat16)
    rows = 2 * mine_t
    r, c = iota((bands * rows, LANES), 0), iota((bands * rows, LANES), 1)
    is_odd = (r % rows) // mine_t
    wanted = 2 * users + 2 * ((r // rows) * mine_t + r % mine_t) + is_odd
    pick = jnp.where(c == wanted, (1 - 2 * is_odd).astype(jnp.float32), 0.0).astype(jnp.bfloat16)
    pick = jnp.concatenate([pick, pick], axis=1)
    half = users // 2
    left = iota((half, LANES), 1) < 2 * users
    for s, factor in enumerate(factors):
        high, low = split(factor * constellation_norm)
        wide = jnp.dot(high, spread, preferred_element_type=jnp.float32) + jnp.dot(
            low, spread, preferred_element_type=jnp.float32
        )
        folded = jnp.where(left, wide[:half], wide[half:])
        for k in range(bands):
            packed[k, s, :half] = folded
        high, low = split(factor)
        weights = jnp.concatenate(
            [jnp.concatenate([high] * copies, axis=0), jnp.concatenate([low] * copies, axis=0)], axis=1
        )
        rotations[s] = lax.dot_general(pick, weights, NT, preferred_element_type=jnp.float32)
        for k in range(bands):
            peer = lax.rem(band + k, bands)
            packed[k, s, half:] = rotations[s, pl.ds(pl.multiple_of(peer * rows, rows), rows), :]
    usends = []
    for k in range(1, bands):
        copy = pltpu.make_async_remote_copy(
            src_ref=packed.at[k], dst_ref=taken.at[k], send_sem=usend_sem.at[k], recv_sem=urecv_sem.at[k],
            device_id={"par": lax.rem(band + k, bands)}, device_id_type=MESH,
        )
        copy.start()
        usends.append(copy)

    sr, sc = iota((LANES, LANES), 0), iota((LANES, LANES), 1)
    suffix = jnp.where((sr // users == sc // users) & (sr >= sc), 1.0 / users, 0.0).astype(jnp.bfloat16)
    suffix = jnp.concatenate([suffix, suffix], axis=0)
    lane_block = lane // users
    for k in range(bands):
        if k:
            usends[k - 1].wait_recv()
        b = lax.rem(band + bands - k, bands)
        box = taken if k else packed
        for s in range(share):
            folded = box[k, s, :half]
            crossed = pltpu.roll(folded, 2 * users, 1)
            first = jnp.concatenate(
                [jnp.where(left, folded, crossed), jnp.where(left, crossed, folded)], axis=0
            )
            second = pltpu.roll(first, users, 1)
            ons, offs = [], []
            for i in range(copies):
                here = lane_block == i
                real, imag = (first, second) if i % 2 == 0 else (second, first)
                real, imag = jnp.where(here, real, 0.0), jnp.where(here, imag, 0.0)
                ons.append(jnp.concatenate([real, imag], axis=1))
                offs.append(jnp.concatenate([-imag, real], axis=1))
            high, low = split(jnp.concatenate(ons + offs, axis=0))
            p = points[b, s]
            mapped = lax.dot_general(p, high, NT, preferred_element_type=jnp.float32) + lax.dot_general(
                p, low, NT, preferred_element_type=jnp.float32
            )
            on = jnp.concatenate([box[k, s, half : half + mine_t]] * pieces, axis=0) - mapped[:, :LANES]
            off = jnp.concatenate([box[k, s, half + mine_t :]] * pieces, axis=0) - mapped[:, LANES:]
            high, low = split(on * on + off * off)
            result = jnp.dot(
                jnp.concatenate([high, low], axis=1), suffix, preferred_element_type=jnp.float32
            )
            for r in range(pieces):
                out_ref[b, s, :, LANES * r : LANES * (r + 1)] = result[mine_t * r : mine_t * (r + 1)]
    for copy in sends + usends:
        copy.wait_send()


def local(propagation_gains, observed_samples, disturbance_variance, retained_branches):
    clusters, bands = lax.axis_size("chain"), lax.axis_size("par")
    _, tones, double_users, antennas = propagation_gains.shape
    users, symbols = double_users // 2, observed_samples.shape[2] // 2
    share, mine_t = tones // clusters, symbols // bands
    pieces = retained_branches.shape[-1] // LANES
    dims = (clusters, bands, users, symbols, share, mine_t, pieces)
    f32, bf16 = jnp.float32, jnp.bfloat16
    vmem, dma = pltpu.VMEM, pltpu.SemaphoreType.DMA
    payload = users // 2 + 2 * mine_t
    return pl.pallas_call(
        functools.partial(kernel, dims),
        out_shape=jax.ShapeDtypeStruct(retained_branches.shape, f32),
        in_specs=[
            pl.BlockSpec(memory_space=pl.ANY),
            pl.BlockSpec(memory_space=pl.ANY),
            pl.BlockSpec(memory_space=pl.ANY),
            pl.BlockSpec(memory_space=pl.ANY),
        ],
        out_specs=pl.BlockSpec(memory_space=pltpu.VMEM),
        scratch_shapes=[
            vmem(disturbance_variance.shape[::-1], f32),
            vmem(retained_branches.shape, jnp.int32),
            vmem((clusters, share, 2 * (users + symbols), antennas), bf16),
            vmem((4, 2 * users, LANES), f32),
            vmem((clusters, share, users, LANES), f32),
            vmem((clusters, share, users, LANES), f32),
            vmem((bands, share, pieces * mine_t, 2 * LANES), bf16),
            vmem((bands, share, payload, LANES), f32),
            vmem((bands, share, payload, LANES), f32),
            vmem((share, bands * 2 * mine_t, LANES), f32),
            dma((2,)), dma((2, clusters)), dma((clusters,)), dma((clusters,)), dma((bands,)), dma((bands,)),
        ],
        compiler_params=pltpu.CompilerParams(collective_id=0, has_side_effects=True),
        name="detect",
    )(disturbance_variance.T, propagation_gains, observed_samples, retained_branches)


def solution(mesh):
    placed = (
        P("par", None, None, "chain"),
        P("par", None, None, "chain"),
        P(None, "chain"),
        P(None, "chain", "par", None),
    )
    return jax.shard_map(
        local, mesh=mesh, in_specs=placed, out_specs=P(None, "chain", "par", None), check_vma=False
    )
```
